256 devices in a mesh: band: 2 (over y), coarse: 8 (over x, core), fine: 16 (over z).
Axes of the slice: x: 4, y: 2, z: 16, core: 2. Of those that a mesh axis runs over, the one named last changes fastest.
The devices are a block of a 4x16x16 slice.
Arguments:
- spectra: float32 [32, 16, 32768], P(None, ('band', 'coarse'), 'fine'), parts along dimension 1, may hold values from 0.2 to 5
Outputs:
- drift_power: float32 [8, 32, 16, 32768], P(None, None, ('band', 'coarse'), 'fine'), parts along dimension 2
The draws below stay inside these ranges and needn't reach their ends.
There are 2 independent parts, one for each index of `band`. The reference program is written for one: setup_inputs(seed, part) draws one part's arguments, and reference() takes and returns one part's arrays. A program takes and returns all parts, laid end to end along the dimension named above; each array names one. Nothing has to cross between parts.
All inputs are finite; a program needn't handle non-finite values.
Results may differ from the reference program's by a relative error of at most 0.00002.
Values sent between devices are 32-bit elements; how exact they have to be, the bound alone decides.
No kernel may reach another device: no remote copies, remote signals or barrier semaphores. Data moves between devices by JAX's collectives and lax.ppermute only.
A program may use at most 64 MiB of HBM per device.

```python
import math
import jax
import jax.numpy as jnp

ROWS = 32
RATES = 8
FINE = 32768
COARSE = 8


def levels(own_key, dims, split, least, top_value):
    gain, own = 1.0, jax.random.fold_in(own_key, 6)
    for axis_at, parts in split:
        draws = jnp.exp(jax.random.uniform(jax.random.fold_in(own, axis_at), (parts,), jnp.float32, least / len(split), top_value / len(split)))
        gain = gain * jnp.repeat(draws, dims[axis_at] // parts).reshape([-1 if axis == axis_at else 1 for axis in range(len(dims))])
    return gain


def setup_inputs(seed: int = 0, part: int = 0) -> dict:
    seeds = jax.random.split(jax.random.key(seed), 2)
    own_keys = jax.random.split(jax.random.fold_in(seeds[1], part), 2)
    return {
        "spectra": jnp.clip(jnp.exp(math.log(5.0) - 3.218876 * jax.random.uniform(own_keys[0], (ROWS, COARSE, FINE), jnp.float32) ** levels(own_keys[0], (ROWS, COARSE, FINE), ((1, 8), (2, 16)), -0.2, 0.2)), 0.2, 5.0),
    }


def shift_left(values, amount):
    if amount == 0:
        return values
    filler = jnp.zeros(values.shape[:-1] + (amount,), values.dtype)
    return jnp.concatenate([values[..., amount:], filler], axis=-1)


def drift_tree(rows_in):
    blocks = rows_in[:, None, :]
    stride = 1
    while stride < rows_in.shape[0]:
        firsts = blocks[0::2]
        seconds = blocks[1::2]
        even_part = jnp.stack([shift_left(seconds[:, position], position) for position in range(stride)], axis=1)
        odd_part = jnp.stack([shift_left(seconds[:, position], position + 1) for position in range(stride)], axis=1)
        joined = jnp.stack([firsts + even_part, firsts + odd_part], axis=2)
        blocks = joined.reshape(firsts.shape[0], 2 * stride, rows_in.shape[1])
        stride = stride * 2
    return blocks[0]


def reference(spectra):
    bandpass = jnp.sum(spectra, axis=1) / COARSE
    inverse = 1.0 / bandpass
    columns = COARSE * FINE
    normed = (spectra * inverse[:, None, :] - 1.0).reshape(ROWS, columns)
    margin = 4 * ROWS
    padded = jnp.pad(normed, ((0, 0), (margin, margin)))
    outputs = []
    for rate_index in range(RATES):
        row_slope = rate_index - RATES // 2
        sheared = jnp.stack([padded[row_index, margin + row_slope * row_index: margin + row_slope * row_index + columns] for row_index in range(ROWS)])
        outputs.append(drift_tree(sheared))
    return jnp.stack(outputs).reshape(RATES, ROWS, COARSE, FINE)
```

```python
import functools

import jax
import jax.numpy as jnp
from jax import lax
from jax.experimental import pallas as pl
from jax.experimental.pallas import tpu as pltpu
from jax.sharding import PartitionSpec as P

RATES = 8
LANES = 128
SUB = 8
VMEM_LIMIT = 36 * 1024 * 1024
APART = (1, 2, 3)


def reverse(i, bits):
    return int(format(i, f"0{bits}b")[::-1], 2)


def plan(rows):
    half, levels, m = RATES // 2, [], 1
    while m < rows:
        size = 2 * m
        level = []
        for key in range(-half * (size - 1), half * (size - 1) + 1):
            q = min(key // (size - 1), half - 1)
            d = key - q * (size - 1)
            level.append((key, q * (m - 1) + d // 2, q * m + d - d // 2))
        levels.append((m, level))
        m = size
    return levels


def drift(rows, chunks, channels):
    half = RATES // 2
    levels = plan(rows)
    bits = len(levels)
    wide = chunks + 2

    def up(n):
        return -(-n // SUB) * SUB

    heights = [up((rows >> lv) * wide) + SUB for lv in range(bits)]
    counts = [2 * half * ((1 << lv) - 1) + 1 for lv in range(bits)]

    def at(start):
        return pl.ds(start, SUB)

    def kernel(x_ref, low_ref, high_ref, lo_ref, hi_ref, end_ref, out_ref, stage, fixed, sems, *bufs):
        trees, turns = bufs[:bits], bufs[bits:]
        lane = lax.broadcasted_iota(jnp.int32, (SUB, LANES), 1)
        line = lane + LANES * lax.broadcasted_iota(jnp.int32, (SUB, LANES), 0)

        base = trees[0]
        for t in range(rows):
            r = reverse(t, bits) * wide
            sums = low_ref if t < rows // 2 else high_ref
            base[0, pl.ds(r, 1), :] = lo_ref[pl.ds(t, 1), :]
            for k in range(0, chunks, SUB):
                inverse = 1.0 / (sums[t % (rows // 2), at(k), :] / channels)
                base[0, at(r + 1 + k), :] = x_ref[t, at(k), :] * inverse - 1.0
            base[0, pl.ds(r + 1 + chunks, 1), :] = hi_ref[pl.ds(t, 1), :]

        def grow(lv, m, level):
            src, dst, turn = trees[lv], trees[lv + 1], turns[lv]
            n = (rows >> (lv + 1)) * wide
            for w, (key, child, s) in enumerate(level):
                a, o = child + half * (m - 1), key + half * (2 * m - 1)
                if s:
                    for r in range(0, n, SUB):
                        turn[w, at(SUB + r), :] = pltpu.roll(src[a, at(n + r), :], -s % LANES, 1)
                for r in range(0, n, SUB):
                    if s == 0:
                        v = src[a, at(n + r), :]
                    elif s > 0:
                        v = lax.select(lane < LANES - s, turn[w, at(SUB + r), :], turn[w, at(SUB + r + 1), :])
                    else:
                        v = lax.select(lane >= -s, turn[w, at(SUB + r), :], turn[w, at(SUB + r - 1), :])
                    dst[o, at(r), :] = src[a, at(r), :] + v

        def apart(run):
            pl.when(end_ref[0] >= 0)(run)

        for lv, (m, level) in enumerate(levels[:-1]):
            step = functools.partial(grow, lv, m, level)
            if lv in APART:
                apart(step)
            else:
                step()

        m = levels[-1][0]
        src, turn = trees[-1], turns[-1]
        copies = []

        def finish(q):
            for d in range(rows):
                w = (q + half) * rows + d
                s = q * m + d - d // 2
                a = q * (m - 1) + d // 2 + half * (m - 1)
                vs = [src[a, at(wide + 1 + k), :] for k in range(0, chunks, SUB)]
                if s > 0:
                    vs[0] = lax.select(line < s, src[a, at(wide + 1 + chunks), :], vs[0])
                if s < 0:
                    vs[-1] = lax.select(line >= SUB * LANES + s, src[a, at(wide + 1 - SUB), :], vs[-1])
                if s:
                    vs = [pltpu.roll(v, -s % LANES, 1) for v in vs]
                    for i, v in enumerate(vs):
                        turn[w, at(SUB + SUB * i), :] = v
                    if s > 0:
                        turn[w, at(SUB + chunks), :] = vs[0]
                        vs = [lax.select(lane < LANES - s, v, turn[w, at(SUB + SUB * i + 1), :]) for i, v in enumerate(vs)]
                    else:
                        turn[w, at(0), :] = vs[-1]
                        vs = [lax.select(lane >= -s, v, turn[w, at(SUB + SUB * i - 1), :]) for i, v in enumerate(vs)]
                for i, v in enumerate(vs):
                    stage[w, at(SUB * i), :] = src[a, at(1 + SUB * i), :] + v

        def send(q):
            part = pl.ds((q + half) * rows, rows)
            copy = pltpu.make_async_copy(stage.at[part], out_ref.at[part], sems.at[q + half])
            copy.start()
            copies.append(copy)

        @apart
        def _():
            for q in range(-half, 0):
                finish(q)

        @pl.when(end_ref[0] > 0)
        def _():
            rate = lax.broadcasted_iota(jnp.int32, (RATES, LANES), 0)
            slope = half - 1 - rate
            blocks = []
            for t in range(rows):
                r = reverse(t, bits) * wide + 1 + chunks
                parts = []
                for k in (2, 1):
                    v = base[0, pl.ds(r - k, 1), :]
                    if t:
                        v = pltpu.roll(v, LANES - (half - 1) * t, 1)
                    v = jnp.broadcast_to(v, (RATES, LANES))
                    step = t
                    if (RATES - 1) * t >= LANES:
                        v = pltpu.roll(v, 0, 1, stride=SUB * 2, stride_axis=0)
                        step = t - SUB * 2
                    if step:
                        v = pltpu.roll(v, 0, 1, stride=step, stride_axis=0)
                    parts.append(v)
                where = lane + slope * t
                v = jnp.where(where < 0, parts[0], jnp.where(where < LANES, parts[1], 0.0))
                blocks.append([v])
            while len(blocks) > 1:
                joined = []
                for first, second in zip(blocks[0::2], blocks[1::2]):
                    block = []
                    for d in range(2 * len(first)):
                        s, v = d - d // 2, second[d // 2]
                        if s:
                            v = jnp.where(lane < LANES - s, pltpu.roll(v, LANES - s, 1), 0.0)
                        block.append(first[d // 2] + v)
                    joined.append(block)
                blocks = joined
            for d in range(rows):
                fixed[...] = blocks[0][d]
                for q in range(-half, 0):
                    stage[(q + half) * rows + d, pl.ds(chunks - 1, 1), :] = fixed[pl.ds(half - 1 - q, 1), :]

        for q in range(-half, 0):
            send(q)
        for q in range(half):
            finish(q)
            send(q)
        for copy in copies:
            copy.wait()

    def call(x, low, high, lo, hi, end):
        f32 = jnp.float32
        paths = RATES * rows
        return pl.pallas_call(
            kernel,
            out_shape=jax.ShapeDtypeStruct((paths, chunks, LANES), f32),
            in_specs=[pl.BlockSpec(memory_space=pltpu.VMEM)] * 5 + [pl.BlockSpec(memory_space=pltpu.SMEM)],
            out_specs=pl.BlockSpec(memory_space=pl.ANY),
            scratch_shapes=[
                pltpu.VMEM((paths, chunks, LANES), f32),
                pltpu.VMEM((RATES, LANES), f32),
                pltpu.SemaphoreType.DMA((RATES,)),
            ]
            + [pltpu.VMEM((counts[lv], heights[lv], LANES), f32) for lv in range(bits)]
            + [pltpu.VMEM((len(level), up((rows >> (lv + 1)) * wide) + 2 * SUB, LANES), f32) for lv, (_, level) in enumerate(levels[:-1])]
            + [pltpu.VMEM((paths, chunks + 2 * SUB, LANES), f32)],
            compiler_params=pltpu.CompilerParams(vmem_limit_bytes=VMEM_LIMIT),
            name="drift",
        )(x, low, high, lo, hi, end)

    return call


def exchange(value, axes, partner):
    count = lax.axis_size(axes)
    return lax.ppermute(value, axes, [(i, partner(i)) for i in range(count) if 0 <= partner(i) < count])


def full_sum(x):
    half = x.shape[0] // 2
    side = lax.axis_index("coarse") % 2
    low, high = x[:half], x[half:]
    own = jnp.where(side == 0, low, high)
    given = jnp.where(side == 0, high, low)
    pair = own + exchange(given, "coarse", lambda i: i ^ 1)
    total = pair
    for k in range(1, lax.axis_size("coarse") // 2):
        total = total + exchange(pair, "coarse", lambda i: i ^ (2 * k))
    other = exchange(total, "coarse", lambda i: i ^ 1)
    return jnp.where(side == 0, total, other), jnp.where(side == 0, other, total)


def on_device(spectra):
    rows, _, columns = spectra.shape
    chunks = columns // LANES
    x = spectra.reshape(rows, chunks, LANES)
    channels = lax.axis_size("coarse") * spectra.shape[1]
    low, high = full_sum(x)
    band = ("coarse", "fine")
    place = lax.axis_index(band)
    odd = place % 2

    def normed(k):
        sums = jnp.concatenate([low[:, k, :], high[:, k, :]], axis=0)
        return x[:, k, :] * (1.0 / (sums / channels)) - 1.0

    first, last = normed(0), normed(-1)
    near = exchange(jnp.where(odd == 1, first, last), band, lambda i: i ^ 1)
    far = exchange(jnp.where(odd == 1, last, first), band, lambda i: i + 1 if i % 2 else i - 1)
    before = jnp.where(odd == 1, near, far)
    after = jnp.where(odd == 1, far, near)
    at_end = (place == lax.axis_size(band) - 1).astype(jnp.int32).reshape(1)
    out = drift(rows, chunks, channels)(x, low, high, before, after, at_end)
    return out.reshape(RATES, rows, 1, columns)


def solution(mesh):
    in_specs = (P(None, ("band", "coarse"), "fine"),)
    out_specs = P(None, None, ("band", "coarse"), "fine")
    return jax.shard_map(
        on_device, mesh=mesh, in_specs=in_specs, out_specs=out_specs, check_vma=False
    )
```

```python
import functools

import jax
import jax.numpy as jnp
from jax import lax
from jax.experimental import pallas as pl
from jax.experimental.pallas import tpu as pltpu
from jax.sharding import PartitionSpec as P

RATES = 8
LANES = 128
SUB = 8
VMEM_LIMIT = 36 * 1024 * 1024
APART = (1, 2, 3)


def reverse(i, bits):
    return int(format(i, f"0{bits}b")[::-1], 2)


def plan(rows):
    half, levels, m = RATES // 2, [], 1
    while m < rows:
        size = 2 * m
        level = []
        for key in range(-half * (size - 1), half * (size - 1) + 1):
            q = min(key // (size - 1), half - 1)
            d = key - q * (size - 1)
            level.append((key, q * (m - 1) + d // 2, q * m + d - d // 2))
        levels.append((m, level))
        m = size
    return levels


def drift(rows, chunks, channels):
    half = RATES // 2
    levels = plan(rows)
    bits = len(levels)
    wide = chunks + 2

    def up(n):
        return -(-n // SUB) * SUB

    heights = [up((rows >> lv) * wide) + SUB for lv in range(bits)]
    counts = [2 * half * ((1 << lv) - 1) + 1 for lv in range(bits)]

    def at(start):
        return pl.ds(start, SUB)

    def kernel(x_ref, low_ref, high_ref, lo_ref, hi_ref, end_ref, out_ref, stage, fixed, sems, *bufs):
        trees, turns = bufs[:bits], bufs[bits:]
        lane = lax.broadcasted_iota(jnp.int32, (SUB, LANES), 1)
        line = lane + LANES * lax.broadcasted_iota(jnp.int32, (SUB, LANES), 0)

        base = trees[0]
        for t in range(rows):
            r = reverse(t, bits) * wide
            sums = low_ref if t < rows // 2 else high_ref
            base[0, pl.ds(r, 1), :] = lo_ref[pl.ds(t, 1), :]
            for k in range(0, chunks, SUB):
                inverse = 1.0 / (sums[t % (rows // 2), at(k), :] / channels)
                base[0, at(r + 1 + k), :] = x_ref[t, at(k), :] * inverse - 1.0
            base[0, pl.ds(r + 1 + chunks, 1), :] = hi_ref[pl.ds(t, 1), :]

        def grow(lv, m, level):
            src, dst, turn = trees[lv], trees[lv + 1], turns[lv]
            n = (rows >> (lv + 1)) * wide
            for w, (key, child, s) in enumerate(level):
                a, o = child + half * (m - 1), key + half * (2 * m - 1)
                if s:
                    for r in range(0, n, SUB):
                        turn[w, at(SUB + r), :] = pltpu.roll(src[a, at(n + r), :], -s % LANES, 1)
                for r in range(0, n, SUB):
                    if s == 0:
                        v = src[a, at(n + r), :]
                    elif s > 0:
                        v = lax.select(lane < LANES - s, turn[w, at(SUB + r), :], turn[w, at(SUB + r + 1), :])
                    else:
                        v = lax.select(lane >= -s, turn[w, at(SUB + r), :], turn[w, at(SUB + r - 1), :])
                    dst[o, at(r), :] = src[a, at(r), :] + v

        def apart(run):
            pl.when(end_ref[0] >= 0)(run)

        for lv, (m, level) in enumerate(levels[:-1]):
            step = functools.partial(grow, lv, m, level)
            if lv in APART:
                apart(step)
            else:
                step()

        m = levels[-1][0]
        src, turn = trees[-1], turns[-1]
        copies = []

        def finish(q):
            for d in range(rows):
                w = (q + half) * rows + d
                s = q * m + d - d // 2
                a = q * (m - 1) + d // 2 + half * (m - 1)
                vs = [src[a, at(wide + 1 + k), :] for k in range(0, chunks, SUB)]
                if s > 0:
                    vs[0] = lax.select(line < s, src[a, at(wide + 1 + chunks), :], vs[0])
                if s < 0:
                    vs[-1] = lax.select(line >= SUB * LANES + s, src[a, at(wide + 1 - SUB), :], vs[-1])
                if s:
                    vs = [pltpu.roll(v, -s % LANES, 1) for v in vs]
                    for i, v in enumerate(vs):
                        turn[w, at(SUB + SUB * i), :] = v
                    if s > 0:
                        turn[w, at(SUB + chunks), :] = vs[0]
                        vs = [lax.select(lane < LANES - s, v, turn[w, at(SUB + SUB * i + 1), :]) for i, v in enumerate(vs)]
                    else:
                        turn[w, at(0), :] = vs[-1]
                        vs = [lax.select(lane >= -s, v, turn[w, at(SUB + SUB * i - 1), :]) for i, v in enumerate(vs)]
                for i, v in enumerate(vs):
                    stage[w, at(SUB * i), :] = src[a, at(1 + SUB * i), :] + v

        def send(q):
            part = pl.ds((q + half) * rows, rows)
            copy = pltpu.make_async_copy(stage.at[part], out_ref.at[part], sems.at[q + half])
            copy.start()
            copies.append(copy)

        @apart
        def _():
            for q in range(-half, 0):
                finish(q)

        @pl.when(end_ref[0] > 0)
        def _():
            rate = lax.broadcasted_iota(jnp.int32, (RATES, LANES), 0)
            slope = half - 1 - rate
            blocks = []
            for t in range(rows):
                r = reverse(t, bits) * wide + 1 + chunks
                parts = []
                for k in (2, 1):
                    v = base[0, pl.ds(r - k, 1), :]
                    if t:
                        v = pltpu.roll(v, LANES - (half - 1) * t, 1)
                    v = jnp.broadcast_to(v, (RATES, LANES))
                    step = t
                    if (RATES - 1) * t >= LANES:
                        v = pltpu.roll(v, 0, 1, stride=SUB * 2, stride_axis=0)
                        step = t - SUB * 2
                    if step:
                        v = pltpu.roll(v, 0, 1, stride=step, stride_axis=0)
                    parts.append(v)
                where = lane + slope * t
                v = jnp.where(where < 0, parts[0], jnp.where(where < LANES, parts[1], 0.0))
                blocks.append([v])
            while len(blocks) > 1:
                joined = []
                for first, second in zip(blocks[0::2], blocks[1::2]):
                    block = []
                    for d in range(2 * len(first)):
                        s, v = d - d // 2, second[d // 2]
                        if s:
                            v = jnp.where(lane < LANES - s, pltpu.roll(v, LANES - s, 1), 0.0)
                        block.append(first[d // 2] + v)
                    joined.append(block)
                blocks = joined
            for d in range(rows):
                fixed[...] = blocks[0][d]
                for q in range(-half, 0):
                    stage[(q + half) * rows + d, pl.ds(chunks - 1, 1), :] = fixed[pl.ds(half - 1 - q, 1), :]

        for q in range(-half, 0):
            send(q)
        for q in range(half):
            finish(q)
            send(q)
        for copy in copies:
            copy.wait()

    def call(x, low, high, lo, hi, end):
        f32 = jnp.float32
        paths = RATES * rows
        return pl.pallas_call(
            kernel,
            out_shape=jax.ShapeDtypeStruct((paths, chunks, LANES), f32),
            in_specs=[pl.BlockSpec(memory_space=pltpu.VMEM)] * 5 + [pl.BlockSpec(memory_space=pltpu.SMEM)],
            out_specs=pl.BlockSpec(memory_space=pl.ANY),
            scratch_shapes=[
                pltpu.VMEM((paths, chunks, LANES), f32),
                pltpu.VMEM((RATES, LANES), f32),
                pltpu.SemaphoreType.DMA((RATES,)),
            ]
            + [pltpu.VMEM((counts[lv], heights[lv], LANES), f32) for lv in range(bits)]
            + [pltpu.VMEM((len(level), up((rows >> (lv + 1)) * wide) + 2 * SUB, LANES), f32) for lv, (_, level) in enumerate(levels[:-1])]
            + [pltpu.VMEM((paths, chunks + 2 * SUB, LANES), f32)],
            compiler_params=pltpu.CompilerParams(vmem_limit_bytes=VMEM_LIMIT),
            name="drift",
        )(x, low, high, lo, hi, end)

    return call


def exchange(value, axes, partner):
    count = lax.axis_size(axes)
    return lax.ppermute(value, axes, [(i, partner(i)) for i in range(count) if 0 <= partner(i) < count])


def full_sum(x):
    half = x.shape[0] // 2
    side = lax.axis_index("coarse") % 2
    low, high = x[:half], x[half:]
    own = jnp.where(side == 0, low, high)
    given = jnp.where(side == 0, high, low)
    pair = own + exchange(given, "coarse", lambda i: i ^ 1)
    total = pair
    for near, far in ((2, 6), (6, 2)):
        total = total + exchange(total, "coarse", lambda i: i ^ (far if i % 2 else near))
    other = exchange(total, "coarse", lambda i: i ^ 1)
    return jnp.where(side == 0, total, other), jnp.where(side == 0, other, total)


def on_device(spectra):
    rows, _, columns = spectra.shape
    chunks = columns // LANES
    x = spectra.reshape(rows, chunks, LANES)
    channels = lax.axis_size("coarse") * spectra.shape[1]
    low, high = full_sum(x)
    band = ("coarse", "fine")
    place = lax.axis_index(band)
    odd = place % 2

    def normed(k):
        sums = jnp.concatenate([low[:, k, :], high[:, k, :]], axis=0)
        return x[:, k, :] * (1.0 / (sums / channels)) - 1.0

    first, last = normed(0), normed(-1)
    near = exchange(jnp.where(odd == 1, first, last), band, lambda i: i ^ 1)
    far = exchange(jnp.where(odd == 1, last, first), band, lambda i: i + 1 if i % 2 else i - 1)
    before = jnp.where(odd == 1, near, far)
    after = jnp.where(odd == 1, far, near)
    at_end = (place == lax.axis_size(band) - 1).astype(jnp.int32).reshape(1)
    out = drift(rows, chunks, channels)(x, low, high, before, after, at_end)
    return out.reshape(RATES, rows, 1, columns)


def solution(mesh):
    in_specs = (P(None, ("band", "coarse"), "fine"),)
    out_specs = P(None, None, ("band", "coarse"), "fine")
    return jax.shard_map(
        on_device, mesh=mesh, in_specs=in_specs, out_specs=out_specs, check_vma=False
    )
```

```python
import functools

import jax
import jax.numpy as jnp
from jax import lax
from jax.experimental import pallas as pl
from jax.experimental.pallas import tpu as pltpu
from jax.sharding import PartitionSpec as P


RATES = 8
LANES = 128
SUB = 8
VMEM_LIMIT = 36 * 1024 * 1024
APART = (1, 2, 3)
INSIDE_FLOPS = 40_000_000


def reverse(i, bits):
    return int(format(i, f"0{bits}b")[::-1], 2)


def plan(rows):
    half, levels, m = RATES // 2, [], 1
    while m < rows:
        size = 2 * m
        level = []
        for key in range(-half * (size - 1), half * (size - 1) + 1):
            q = min(key // (size - 1), half - 1)
            d = key - q * (size - 1)
            level.append((key, q * (m - 1) + d // 2, q * m + d - d // 2))
        levels.append((m, level))
        m = size
    return levels


def inside(rows, chunks, channels):
    half = RATES // 2
    levels = plan(rows)
    bits = len(levels)
    wide = chunks + 2

    def up(n):
        return -(-n // SUB) * SUB

    heights = [up((rows >> lv) * wide) + SUB for lv in range(bits)]
    counts = [2 * half * ((1 << lv) - 1) + 1 for lv in range(bits)]

    def at(start):
        return pl.ds(start, SUB)

    def kernel(x_ref, low_ref, high_ref, end_ref, stage, fixed, *bufs):
        trees, turns = bufs[:bits], bufs[bits:]
        lane = lax.broadcasted_iota(jnp.int32, (SUB, LANES), 1)
        line = lane + LANES * lax.broadcasted_iota(jnp.int32, (SUB, LANES), 0)

        none = jnp.zeros((1, LANES), jnp.float32)
        base = trees[0]
        for t in range(rows):
            r = reverse(t, bits) * wide
            base[0, pl.ds(r, 1), :] = none
            for k in range(0, chunks, SUB):
                sums = low_ref if k < chunks // 2 else high_ref
                inverse = 1.0 / (sums[t, at(k % (chunks // 2)), :] / channels)
                base[0, at(r + 1 + k), :] = x_ref[t, at(k), :] * inverse - 1.0
            base[0, pl.ds(r + 1 + chunks, 1), :] = none

        def grow(lv, m, level):
            src, dst, turn = trees[lv], trees[lv + 1], turns[lv]
            n = (rows >> (lv + 1)) * wide
            for w, (key, child, s) in enumerate(level):
                a, o = child + half * (m - 1), key + half * (2 * m - 1)
                if s:
                    for r in range(0, n, SUB):
                        turn[w, at(SUB + r), :] = pltpu.roll(src[a, at(n + r), :], -s % LANES, 1)
                for r in range(0, n, SUB):
                    if s == 0:
                        v = src[a, at(n + r), :]
                    elif s > 0:
                        v = lax.select(lane < LANES - s, turn[w, at(SUB + r), :], turn[w, at(SUB + r + 1), :])
                    else:
                        v = lax.select(lane >= -s, turn[w, at(SUB + r), :], turn[w, at(SUB + r - 1), :])
                    dst[o, at(r), :] = src[a, at(r), :] + v

        def apart(run):
            pl.when(end_ref[0] >= 0)(run)

        for lv, (m, level) in enumerate(levels[:-1]):
            step = functools.partial(grow, lv, m, level)
            if lv in APART:
                apart(step)
            else:
                step()

        m = levels[-1][0]
        src, turn = trees[-1], turns[-1]

        def finish(q):
            for d in range(rows):
                w = (q + half) * rows + d
                s = q * m + d - d // 2
                a = q * (m - 1) + d // 2 + half * (m - 1)
                vs = [src[a, at(wide + 1 + k), :] for k in range(0, chunks, SUB)]
                if s > 0:
                    vs[0] = lax.select(line < s, src[a, at(wide + 1 + chunks), :], vs[0])
                if s < 0:
                    vs[-1] = lax.select(line >= SUB * LANES + s, src[a, at(wide + 1 - SUB), :], vs[-1])
                if s:
                    vs = [pltpu.roll(v, -s % LANES, 1) for v in vs]
                    for i, v in enumerate(vs):
                        turn[w, at(SUB + SUB * i), :] = v
                    if s > 0:
                        turn[w, at(SUB + chunks), :] = vs[0]
                        vs = [lax.select(lane < LANES - s, v, turn[w, at(SUB + SUB * i + 1), :]) for i, v in enumerate(vs)]
                    else:
                        turn[w, at(0), :] = vs[-1]
                        vs = [lax.select(lane >= -s, v, turn[w, at(SUB + SUB * i - 1), :]) for i, v in enumerate(vs)]
                for i, v in enumerate(vs):
                    stage[w, at(SUB * i), :] = src[a, at(1 + SUB * i), :] + v

        @apart
        def _():
            for q in range(-half, 0):
                finish(q)

        @pl.when(end_ref[0] > 0)
        def _():
            rate = lax.broadcasted_iota(jnp.int32, (RATES, LANES), 0)
            slope = half - 1 - rate
            blocks = []
            for t in range(rows):
                r = reverse(t, bits) * wide + 1 + chunks
                parts = []
                for k in (2, 1):
                    v = base[0, pl.ds(r - k, 1), :]
                    if t:
                        v = pltpu.roll(v, LANES - (half - 1) * t, 1)
                    v = jnp.broadcast_to(v, (RATES, LANES))
                    step = t
                    if (RATES - 1) * t >= LANES:
                        v = pltpu.roll(v, 0, 1, stride=SUB * 2, stride_axis=0)
                        step = t - SUB * 2
                    if step:
                        v = pltpu.roll(v, 0, 1, stride=step, stride_axis=0)
                    parts.append(v)
                where = lane + slope * t
                v = jnp.where(where < 0, parts[0], jnp.where(where < LANES, parts[1], 0.0))
                blocks.append([v])
            while len(blocks) > 1:
                joined = []
                for first, second in zip(blocks[0::2], blocks[1::2]):
                    block = []
                    for d in range(2 * len(first)):
                        s, v = d - d // 2, second[d // 2]
                        if s:
                            v = jnp.where(lane < LANES - s, pltpu.roll(v, LANES - s, 1), 0.0)
                        block.append(first[d // 2] + v)
                    joined.append(block)
                blocks = joined
            for d in range(rows):
                fixed[...] = blocks[0][d]
                for q in range(-half, 0):
                    stage[(q + half) * rows + d, pl.ds(chunks - 1, 1), :] = fixed[pl.ds(half - 1 - q, 1), :]

        for q in range(half):
            finish(q)

    def call(x, low, high, end):
        f32 = jnp.float32
        paths = RATES * rows
        return pl.pallas_call(
            kernel,
            out_shape=jax.ShapeDtypeStruct((paths, chunks, LANES), f32),
            in_specs=[pl.BlockSpec(memory_space=pltpu.VMEM)] * 3 + [pl.BlockSpec(memory_space=pltpu.SMEM)],
            out_specs=pl.BlockSpec(memory_space=pltpu.VMEM),
            scratch_shapes=[pltpu.VMEM((RATES, LANES), f32)]
            + [pltpu.VMEM((counts[lv], heights[lv], LANES), f32) for lv in range(bits)]
            + [pltpu.VMEM((len(level), up((rows >> (lv + 1)) * wide) + 2 * SUB, LANES), f32) for lv, (_, level) in enumerate(levels[:-1])]
            + [pltpu.VMEM((paths, chunks + 2 * SUB, LANES), f32)],
            compiler_params=pltpu.CompilerParams(vmem_limit_bytes=VMEM_LIMIT),
            cost_estimate=pl.CostEstimate(flops=INSIDE_FLOPS, bytes_accessed=4 * paths * chunks * LANES, transcendentals=0),
            name="inside",
        )(x, low, high, end)

    return call


def edges(rows, chunks):
    half = RATES // 2
    levels = plan(rows)
    bits = len(levels)

    def up(n):
        return -(-n // SUB) * SUB

    def at(start):
        return pl.ds(start, SUB)

    heights = [up((rows >> lv) * 2) + SUB for lv in range(bits)]
    counts = [2 * half * ((1 << lv) - 1) + 2 for lv in range(bits)]

    def kernel(lo_ref, hi_ref, stage_ref, stage, out_ref, sems, *bufs):
        trees, turns = bufs[:bits], bufs[bits:]
        lane = lax.broadcasted_iota(jnp.int32, (SUB, LANES), 1)
        none = jnp.zeros((1, LANES), jnp.float32)
        for t in range(rows):
            r = 2 * reverse(t, bits)
            trees[0][0, pl.ds(r, 1), :] = lo_ref[pl.ds(t, 1), :]
            trees[0][0, pl.ds(r + 1, 1), :] = none
            trees[0][1, pl.ds(r, 1), :] = none
            trees[0][1, pl.ds(r + 1, 1), :] = hi_ref[pl.ds(t, 1), :]

        def place(key, m, above):
            return key + half * (m - 1) + above

        def shifted(turn, w, r, s):
            if s > 0:
                return lax.select(lane < LANES - s, turn[w, at(SUB + r), :], turn[w, at(SUB + r + 1), :])
            return lax.select(lane >= -s, turn[w, at(SUB + r), :], turn[w, at(SUB + r - 1), :])

        for lv, (m, level) in enumerate(levels[:-1]):
            src, dst, turn = trees[lv], trees[lv + 1], turns[lv]
            n = (rows >> (lv + 1)) * 2
            sides = [(key, child, s, 0) for key, child, s in level if key <= 0]
            sides += [(key, child, s, 1) for key, child, s in level if key >= 0]
            for key, child, s, above in sides:
                a, w = place(child, m, above), place(key, 2 * m, above)
                for r in range(0, n, SUB):
                    v = src[a, at(n + r), :]
                    if s:
                        turn[w, at(SUB + r), :] = pltpu.roll(v, -s % LANES, 1)
                for r in range(0, n, SUB):
                    v = shifted(turn, w, r, s) if s else src[a, at(n + r), :]
                    dst[w, at(r), :] = src[a, at(r), :] + v

        m = levels[-1][0]
        src, turn = trees[-1], turns[-1]
        copies = []
        for q in range(-half, half):
            above = int(q >= 0)
            for d in range(rows):
                w = (q + half) * rows + d
                s = q * m + d - d // 2
                a = place(q * (m - 1) + d // 2, m, above)
                v = src[a, at(2), :]
                if s:
                    turn[w, at(SUB), :] = pltpu.roll(v, -s % LANES, 1)
                    v = shifted(turn, w, 0, s)
                v = src[a, at(0), :] + v
                row, k = (0, chunks - 1) if above else (1, 0)
                stage[w, pl.ds(k, 1), :] = stage_ref[w, pl.ds(k, 1), :] + v[row : row + 1]
            part = pl.ds((q + half) * rows, rows)
            copy = pltpu.make_async_copy(stage.at[part], out_ref.at[part], sems.at[q + half])
            copy.start()
            copies.append(copy)
        for copy in copies:
            copy.wait()

    def call(lo, hi, stage):
        f32 = jnp.float32
        paths = RATES * rows
        shape = jax.ShapeDtypeStruct((paths, chunks, LANES), f32)
        return pl.pallas_call(
            kernel,
            out_shape=(shape, shape),
            in_specs=[pl.BlockSpec(memory_space=pltpu.VMEM)] * 3,
            out_specs=(pl.BlockSpec(memory_space=pltpu.VMEM), pl.BlockSpec(memory_space=pl.ANY)),
            scratch_shapes=[pltpu.SemaphoreType.DMA((RATES,))]
            + [pltpu.VMEM((counts[lv], heights[lv], LANES), f32) for lv in range(bits)]
            + [pltpu.VMEM((counts[lv + 1], up((rows >> (lv + 1)) * 2) + 2 * SUB, LANES), f32) for lv in range(bits - 1)]
            + [pltpu.VMEM((paths, 3 * SUB, LANES), f32)],
            input_output_aliases={2: 0},
            compiler_params=pltpu.CompilerParams(vmem_limit_bytes=VMEM_LIMIT),
            name="edges",
        )(lo, hi, stage)[1]

    return call


def exchange(value, axes, partner):
    pairs = [(i, partner(i)) for i in range(lax.axis_size(axes))]
    return lax.ppermute(value, axes, [(i, j) for i, j in pairs if j is not None])


def search(spectra):
    rows, _, columns = spectra.shape
    chunks = columns // LANES
    half = chunks // 2
    x = spectra.reshape(rows, chunks, LANES)
    channels = lax.axis_size("coarse") * spectra.shape[1]
    band, depth = ("coarse", "fine"), lax.axis_size("fine")
    place = lax.axis_index(band)
    side = lax.axis_index("coarse") % 2
    upper = side == 1

    own = jnp.where(upper, x[:, half:], x[:, :half])
    given = exchange(jnp.where(upper, x[:, :half], x[:, half:]), "coarse", lambda i: i ^ 1)
    total = own + given
    for near, far in ((2, 6), (6, 2)):
        total = total + exchange(total, "coarse", lambda i: i ^ (far if i % 2 else near))
    other = exchange(total, "coarse", lambda i: i ^ 1)

    def edge(v):
        return jnp.where(upper, v[:, -1], v[:, 0])

    inverse = 1.0 / (edge(total) / channels)
    mine, others = edge(own) * inverse - 1.0, edge(given) * inverse - 1.0
    at_turn = lax.axis_index("fine") == jnp.where(upper, depth - 1, 0)

    def along(i, cross):
        c, z = divmod(i, depth)
        step = 1 if c % 2 else -1
        if 0 <= z + step < depth:
            return (c ^ cross) * depth + z + step
        c += step * cross
        return c * depth + (z + step) % depth if 0 <= c < lax.axis_size("coarse") else None

    same = exchange(jnp.where(at_turn, others, mine), band, lambda i: along(i, 0))
    crossed = exchange(jnp.where(at_turn, mine, others), band, lambda i: along(i, 1))
    before, after = jnp.where(upper, same, crossed), jnp.where(upper, crossed, same)

    low, high = jnp.where(upper, other, total), jnp.where(upper, total, other)
    at_end = (place == lax.axis_size(band) - 1).astype(jnp.int32).reshape(1)
    stage = inside(rows, chunks, channels)(x, low, high, at_end)
    out = edges(rows, chunks)(before, after, stage)
    return out.reshape(RATES, rows, 1, columns)


def solution(mesh):
    in_specs = (P(None, ("band", "coarse"), "fine"),)
    out_specs = P(None, None, ("band", "coarse"), "fine")
    return jax.shard_map(search, mesh=mesh, in_specs=in_specs, out_specs=out_specs, check_vma=False)
```

```python
import jax
import jax.numpy as jnp
from jax import lax
from jax.experimental import pallas as pl
from jax.experimental.pallas import tpu as pltpu
from jax.sharding import PartitionSpec as P


RATES = 8
LANES = 128
SUB = 8
VMEM_LIMIT = 36 * 1024 * 1024
INSIDE_FLOPS = 40_000_000


def reverse(i, bits):
    return int(format(i, f"0{bits}b")[::-1], 2)


def plan(rows):
    half, levels, m = RATES // 2, [], 1
    while m < rows:
        size = 2 * m
        level = []
        for key in range(-half * (size - 1), half * (size - 1) + 1):
            q = min(key // (size - 1), half - 1)
            d = key - q * (size - 1)
            level.append((key, q * (m - 1) + d // 2, q * m + d - d // 2))
        levels.append((m, level))
        m = size
    return levels


def inside(rows, chunks, channels):
    half = RATES // 2
    levels = plan(rows)
    bits = len(levels)
    wide = chunks + 2

    def up(n):
        return -(-n // SUB) * SUB

    heights = [up((rows >> lv) * wide) + SUB for lv in range(bits)]
    counts = [2 * half * ((1 << lv) - 1) + 1 for lv in range(bits)]

    def at(start):
        return pl.ds(start, SUB)

    def kernel(x_ref, low_ref, high_ref, end_ref, stage, fixed, *bufs):
        trees, turns = bufs[:bits], bufs[bits:]
        lane = lax.broadcasted_iota(jnp.int32, (SUB, LANES), 1)
        line = lane + LANES * lax.broadcasted_iota(jnp.int32, (SUB, LANES), 0)

        none = jnp.zeros((1, LANES), jnp.float32)
        base = trees[0]
        for t in range(rows):
            r = reverse(t, bits) * wide
            base[0, pl.ds(r, 1), :] = none
            for k in range(0, chunks, SUB):
                sums = low_ref if k < chunks // 2 else high_ref
                inverse = 1.0 / (sums[t, at(k % (chunks // 2)), :] / channels)
                base[0, at(r + 1 + k), :] = x_ref[t, at(k), :] * inverse - 1.0
            base[0, pl.ds(r + 1 + chunks, 1), :] = none

        def grow(lv, m, level):
            src, dst, turn = trees[lv], trees[lv + 1], turns[lv]
            n = (rows >> (lv + 1)) * wide
            for w, (key, child, s) in enumerate(level):
                a, o = child + half * (m - 1), key + half * (2 * m - 1)
                if s:
                    for r in range(0, n, SUB):
                        turn[w, at(SUB + r), :] = pltpu.roll(src[a, at(n + r), :], -s % LANES, 1)
                for r in range(0, n, SUB):
                    if s == 0:
                        v = src[a, at(n + r), :]
                    elif s > 0:
                        v = lax.select(lane < LANES - s, turn[w, at(SUB + r), :], turn[w, at(SUB + r + 1), :])
                    else:
                        v = lax.select(lane >= -s, turn[w, at(SUB + r), :], turn[w, at(SUB + r - 1), :])
                    dst[o, at(r), :] = src[a, at(r), :] + v

        for lv, (m, level) in enumerate(levels[:-1]):
            grow(lv, m, level)

        m = levels[-1][0]
        src, turn = trees[-1], turns[-1]

        def finish(q):
            for d in range(rows):
                w = (q + half) * rows + d
                s = q * m + d - d // 2
                a = q * (m - 1) + d // 2 + half * (m - 1)
                vs = [src[a, at(wide + 1 + k), :] for k in range(0, chunks, SUB)]
                if s > 0:
                    vs[0] = lax.select(line < s, src[a, at(wide + 1 + chunks), :], vs[0])
                if s < 0:
                    vs[-1] = lax.select(line >= SUB * LANES + s, src[a, at(wide + 1 - SUB), :], vs[-1])
                if s:
                    vs = [pltpu.roll(v, -s % LANES, 1) for v in vs]
                    for i, v in enumerate(vs):
                        turn[w, at(SUB + SUB * i), :] = v
                    if s > 0:
                        turn[w, at(SUB + chunks), :] = vs[0]
                        vs = [lax.select(lane < LANES - s, v, turn[w, at(SUB + SUB * i + 1), :]) for i, v in enumerate(vs)]
                    else:
                        turn[w, at(0), :] = vs[-1]
                        vs = [lax.select(lane >= -s, v, turn[w, at(SUB + SUB * i - 1), :]) for i, v in enumerate(vs)]
                for i, v in enumerate(vs):
                    stage[w, at(SUB * i), :] = src[a, at(1 + SUB * i), :] + v

        for q in range(-half, 0):
            finish(q)

        @pl.when(end_ref[0] > 0)
        def _():
            rate = lax.broadcasted_iota(jnp.int32, (RATES, LANES), 0)
            slope = half - 1 - rate
            blocks = []
            for t in range(rows):
                r = reverse(t, bits) * wide + 1 + chunks
                parts = []
                for k in (2, 1):
                    v = base[0, pl.ds(r - k, 1), :]
                    if t:
                        v = pltpu.roll(v, LANES - (half - 1) * t, 1)
                    v = jnp.broadcast_to(v, (RATES, LANES))
                    step = t
                    if (RATES - 1) * t >= LANES:
                        v = pltpu.roll(v, 0, 1, stride=SUB * 2, stride_axis=0)
                        step = t - SUB * 2
                    if step:
                        v = pltpu.roll(v, 0, 1, stride=step, stride_axis=0)
                    parts.append(v)
                where = lane + slope * t
                v = jnp.where(where < 0, parts[0], jnp.where(where < LANES, parts[1], 0.0))
                blocks.append([v])
            while len(blocks) > 1:
                joined = []
                for first, second in zip(blocks[0::2], blocks[1::2]):
                    block = []
                    for d in range(2 * len(first)):
                        s, v = d - d // 2, second[d // 2]
                        if s:
                            v = jnp.where(lane < LANES - s, pltpu.roll(v, LANES - s, 1), 0.0)
                        block.append(first[d // 2] + v)
                    joined.append(block)
                blocks = joined
            for d in range(rows):
                fixed[...] = blocks[0][d]
                for q in range(-half, 0):
                    stage[(q + half) * rows + d, pl.ds(chunks - 1, 1), :] = fixed[pl.ds(half - 1 - q, 1), :]

        for q in range(half):
            finish(q)

    def call(x, low, high, end):
        f32 = jnp.float32
        paths = RATES * rows
        return pl.pallas_call(
            kernel,
            out_shape=jax.ShapeDtypeStruct((paths, chunks, LANES), f32),
            in_specs=[pl.BlockSpec(memory_space=pltpu.VMEM)] * 3 + [pl.BlockSpec(memory_space=pltpu.SMEM)],
            out_specs=pl.BlockSpec(memory_space=pltpu.VMEM),
            scratch_shapes=[pltpu.VMEM((RATES, LANES), f32)]
            + [pltpu.VMEM((counts[lv], heights[lv], LANES), f32) for lv in range(bits)]
            + [pltpu.VMEM((len(level), up((rows >> (lv + 1)) * wide) + 2 * SUB, LANES), f32) for lv, (_, level) in enumerate(levels[:-1])]
            + [pltpu.VMEM((paths, chunks + 2 * SUB, LANES), f32)],
            compiler_params=pltpu.CompilerParams(vmem_limit_bytes=VMEM_LIMIT),
            cost_estimate=pl.CostEstimate(flops=INSIDE_FLOPS, bytes_accessed=4 * paths * chunks * LANES, transcendentals=0),
            name="inside",
        )(x, low, high, end)

    return call


def edges(rows, chunks):
    half = RATES // 2
    levels = plan(rows)
    bits = len(levels)

    def up(n):
        return -(-n // SUB) * SUB

    def at(start):
        return pl.ds(start, SUB)

    heights = [up((rows >> lv) * 2) + SUB for lv in range(bits)]
    counts = [2 * half * ((1 << lv) - 1) + 2 for lv in range(bits)]

    def kernel(lo_ref, hi_ref, stage_ref, stage, out_ref, sems, *bufs):
        trees, turns = bufs[:bits], bufs[bits:]
        lane = lax.broadcasted_iota(jnp.int32, (SUB, LANES), 1)
        none = jnp.zeros((1, LANES), jnp.float32)
        for t in range(rows):
            r = 2 * reverse(t, bits)
            trees[0][0, pl.ds(r, 1), :] = lo_ref[pl.ds(t, 1), :]
            trees[0][0, pl.ds(r + 1, 1), :] = none
            trees[0][1, pl.ds(r, 1), :] = none
            trees[0][1, pl.ds(r + 1, 1), :] = hi_ref[pl.ds(t, 1), :]

        def place(key, m, above):
            return key + half * (m - 1) + above

        def shifted(turn, w, r, s):
            if s > 0:
                return lax.select(lane < LANES - s, turn[w, at(SUB + r), :], turn[w, at(SUB + r + 1), :])
            return lax.select(lane >= -s, turn[w, at(SUB + r), :], turn[w, at(SUB + r - 1), :])

        for lv, (m, level) in enumerate(levels[:-1]):
            src, dst, turn = trees[lv], trees[lv + 1], turns[lv]
            n = (rows >> (lv + 1)) * 2
            sides = [(key, child, s, 0) for key, child, s in level if key <= 0]
            sides += [(key, child, s, 1) for key, child, s in level if key >= 0]
            for key, child, s, above in sides:
                a, w = place(child, m, above), place(key, 2 * m, above)
                for r in range(0, n, SUB):
                    v = src[a, at(n + r), :]
                    if s:
                        turn[w, at(SUB + r), :] = pltpu.roll(v, -s % LANES, 1)
                for r in range(0, n, SUB):
                    v = shifted(turn, w, r, s) if s else src[a, at(n + r), :]
                    dst[w, at(r), :] = src[a, at(r), :] + v

        m = levels[-1][0]
        src, turn = trees[-1], turns[-1]
        copies = []
        for q in range(-half, half):
            above = int(q >= 0)
            for d in range(rows):
                w = (q + half) * rows + d
                s = q * m + d - d // 2
                a = place(q * (m - 1) + d // 2, m, above)
                v = src[a, at(2), :]
                if s:
                    turn[w, at(SUB), :] = pltpu.roll(v, -s % LANES, 1)
                    v = shifted(turn, w, 0, s)
                v = src[a, at(0), :] + v
                row, k = (0, chunks - 1) if above else (1, 0)
                stage[w, pl.ds(k, 1), :] = stage_ref[w, pl.ds(k, 1), :] + v[row : row + 1]
            part = pl.ds((q + half) * rows, rows)
            copy = pltpu.make_async_copy(stage.at[part], out_ref.at[part], sems.at[q + half])
            copy.start()
            copies.append(copy)
        for copy in copies:
            copy.wait()

    def call(lo, hi, stage):
        f32 = jnp.float32
        paths = RATES * rows
        shape = jax.ShapeDtypeStruct((paths, chunks, LANES), f32)
        return pl.pallas_call(
            kernel,
            out_shape=(shape, shape),
            in_specs=[pl.BlockSpec(memory_space=pltpu.VMEM)] * 3,
            out_specs=(pl.BlockSpec(memory_space=pltpu.VMEM), pl.BlockSpec(memory_space=pl.ANY)),
            scratch_shapes=[pltpu.SemaphoreType.DMA((RATES,))]
            + [pltpu.VMEM((counts[lv], heights[lv], LANES), f32) for lv in range(bits)]
            + [pltpu.VMEM((counts[lv + 1], up((rows >> (lv + 1)) * 2) + 2 * SUB, LANES), f32) for lv in range(bits - 1)]
            + [pltpu.VMEM((paths, 3 * SUB, LANES), f32)],
            input_output_aliases={2: 0},
            compiler_params=pltpu.CompilerParams(vmem_limit_bytes=VMEM_LIMIT),
            name="edges",
        )(lo, hi, stage)[1]

    return call


def exchange(value, axes, partner):
    pairs = [(i, partner(i)) for i in range(lax.axis_size(axes))]
    return lax.ppermute(value, axes, [(i, j) for i, j in pairs if j is not None])


def search(spectra):
    rows, _, columns = spectra.shape
    chunks = columns // LANES
    half = chunks // 2
    x = spectra.reshape(rows, chunks, LANES)
    channels = lax.axis_size("coarse") * spectra.shape[1]
    band = ("coarse", "fine")
    place = lax.axis_index(band)
    side = lax.axis_index("coarse") % 2
    upper = side == 1

    own = jnp.where(upper, x[:, half:], x[:, :half])
    total = own + exchange(jnp.where(upper, x[:, :half], x[:, half:]), "coarse", lambda i: i ^ 1)

    count = lax.axis_size(band)
    odd = place % 2 == 1
    first, last, total = lax.optimization_barrier((x[:, 0], x[:, -1], total))
    even_rim = exchange(jnp.where(odd, first, last), band, lambda i: i ^ 1)
    odd_rim = exchange(jnp.where(odd, last, first), band, lambda i: (i + (1 if i % 2 else -1)) % count)
    rim = jnp.stack([jnp.where(odd, even_rim, odd_rim), jnp.where(odd, odd_rim, even_rim)])
    rim_sum = rim
    for cross in (1, 2, 6):
        rim_sum = rim_sum + exchange(rim_sum, "coarse", lambda i: i ^ cross)
    inside_band = jnp.stack([place > 0, place < count - 1])[:, None, None]
    rim = jnp.where(inside_band, rim * (1.0 / (rim_sum / channels)) - 1.0, 0.0)

    for near, far in ((2, 6), (6, 2)):
        total = total + exchange(total, "coarse", lambda i: i ^ (far if i % 2 else near))
    other = exchange(total, "coarse", lambda i: i ^ 1)
    low, high = jnp.where(upper, other, total), jnp.where(upper, total, other)
    at_end = (place == count - 1).astype(jnp.int32).reshape(1)
    stage = inside(rows, chunks, channels)(x, low, high, at_end)
    out = edges(rows, chunks)(rim[0], rim[1], stage)
    return out.reshape(RATES, rows, 1, columns)


def solution(mesh):
    in_specs = (P(None, ("band", "coarse"), "fine"),)
    out_specs = P(None, None, ("band", "coarse"), "fine")
    return jax.shard_map(search, mesh=mesh, in_specs=in_specs, out_specs=out_specs, check_vma=False)
```

```python
import jax
import jax.numpy as jnp
from jax import lax
from jax.experimental import pallas as pl
from jax.experimental.pallas import tpu as pltpu
from jax.sharding import PartitionSpec as P


RATES = 8
LANES = 128
SUB = 8
VMEM_LIMIT = 36 * 1024 * 1024
INSIDE_FLOPS = 40_000_000


def reverse(i, bits):
    return int(format(i, f"0{bits}b")[::-1], 2)


def plan(rows):
    half, levels, m = RATES // 2, [], 1
    while m < rows:
        size = 2 * m
        level = []
        for key in range(-half * (size - 1), half * (size - 1) + 1):
            q = min(key // (size - 1), half - 1)
            d = key - q * (size - 1)
            level.append((key, q * (m - 1) + d // 2, q * m + d - d // 2))
        levels.append((m, level))
        m = size
    return levels


def inside(rows, chunks, channels):
    half = RATES // 2
    levels = plan(rows)
    bits = len(levels)
    wide = chunks + 2

    def up(n):
        return -(-n // SUB) * SUB

    heights = [up((rows >> lv) * wide) + SUB for lv in range(bits)]
    counts = [2 * half * ((1 << lv) - 1) + 1 for lv in range(bits)]

    def at(start):
        return pl.ds(start, SUB)

    def kernel(x_ref, low_ref, high_ref, end_ref, stage, fixed, *bufs):
        trees, turns = bufs[:bits], bufs[bits:]
        lane = lax.broadcasted_iota(jnp.int32, (SUB, LANES), 1)
        line = lane + LANES * lax.broadcasted_iota(jnp.int32, (SUB, LANES), 0)

        none = jnp.zeros((1, LANES), jnp.float32)
        base = trees[0]
        for t in range(rows):
            r = reverse(t, bits) * wide
            base[0, pl.ds(r, 1), :] = none
            for k in range(0, chunks, SUB):
                sums = low_ref if k < chunks // 2 else high_ref
                inverse = 1.0 / (sums[t, at(k % (chunks // 2)), :] / channels)
                base[0, at(r + 1 + k), :] = x_ref[t, at(k), :] * inverse - 1.0
            base[0, pl.ds(r + 1 + chunks, 1), :] = none

        def grow(lv, m, level):
            src, dst, turn = trees[lv], trees[lv + 1], turns[lv]
            n = (rows >> (lv + 1)) * wide
            for w, (key, child, s) in enumerate(level):
                a, o = child + half * (m - 1), key + half * (2 * m - 1)
                if s:
                    for r in range(0, n, SUB):
                        turn[w, at(SUB + r), :] = pltpu.roll(src[a, at(n + r), :], -s % LANES, 1)
                for r in range(0, n, SUB):
                    if s == 0:
                        v = src[a, at(n + r), :]
                    elif s > 0:
                        v = lax.select(lane < LANES - s, turn[w, at(SUB + r), :], turn[w, at(SUB + r + 1), :])
                    else:
                        v = lax.select(lane >= -s, turn[w, at(SUB + r), :], turn[w, at(SUB + r - 1), :])
                    dst[o, at(r), :] = src[a, at(r), :] + v

        for lv, (m, level) in enumerate(levels[:-1]):
            grow(lv, m, level)

        m = levels[-1][0]
        src, turn = trees[-1], turns[-1]

        def finish(q):
            for d in range(rows):
                w = (q + half) * rows + d
                s = q * m + d - d // 2
                a = q * (m - 1) + d // 2 + half * (m - 1)
                vs = [src[a, at(wide + 1 + k), :] for k in range(0, chunks, SUB)]
                if s > 0:
                    vs[0] = lax.select(line < s, src[a, at(wide + 1 + chunks), :], vs[0])
                if s < 0:
                    vs[-1] = lax.select(line >= SUB * LANES + s, src[a, at(wide + 1 - SUB), :], vs[-1])
                if s:
                    vs = [pltpu.roll(v, -s % LANES, 1) for v in vs]
                    for i, v in enumerate(vs):
                        turn[w, at(SUB + SUB * i), :] = v
                    if s > 0:
                        turn[w, at(SUB + chunks), :] = vs[0]
                        vs = [lax.select(lane < LANES - s, v, turn[w, at(SUB + SUB * i + 1), :]) for i, v in enumerate(vs)]
                    else:
                        turn[w, at(0), :] = vs[-1]
                        vs = [lax.select(lane >= -s, v, turn[w, at(SUB + SUB * i - 1), :]) for i, v in enumerate(vs)]
                for i, v in enumerate(vs):
                    stage[w, at(SUB * i), :] = src[a, at(1 + SUB * i), :] + v

        for q in range(-half, 0):
            finish(q)

        @pl.when(end_ref[0] > 0)
        def _():
            rate = lax.broadcasted_iota(jnp.int32, (RATES, LANES), 0)
            slope = half - 1 - rate
            blocks = []
            for t in range(rows):
                r = reverse(t, bits) * wide + 1 + chunks
                parts = []
                for k in (2, 1):
                    v = base[0, pl.ds(r - k, 1), :]
                    if t:
                        v = pltpu.roll(v, LANES - (half - 1) * t, 1)
                    v = jnp.broadcast_to(v, (RATES, LANES))
                    step = t
                    if (RATES - 1) * t >= LANES:
                        v = pltpu.roll(v, 0, 1, stride=SUB * 2, stride_axis=0)
                        step = t - SUB * 2
                    if step:
                        v = pltpu.roll(v, 0, 1, stride=step, stride_axis=0)
                    parts.append(v)
                where = lane + slope * t
                v = jnp.where(where < 0, parts[0], jnp.where(where < LANES, parts[1], 0.0))
                blocks.append([v])
            while len(blocks) > 1:
                joined = []
                for first, second in zip(blocks[0::2], blocks[1::2]):
                    block = []
                    for d in range(2 * len(first)):
                        s, v = d - d // 2, second[d // 2]
                        if s:
                            v = jnp.where(lane < LANES - s, pltpu.roll(v, LANES - s, 1), 0.0)
                        block.append(first[d // 2] + v)
                    joined.append(block)
                blocks = joined
            for d in range(rows):
                fixed[...] = blocks[0][d]
                for q in range(-half, 0):
                    stage[(q + half) * rows + d, pl.ds(chunks - 1, 1), :] = fixed[pl.ds(half - 1 - q, 1), :]

        for q in range(half):
            finish(q)

    def call(x, low, high, end):
        f32 = jnp.float32
        paths = RATES * rows
        return pl.pallas_call(
            kernel,
            out_shape=jax.ShapeDtypeStruct((paths, chunks, LANES), f32),
            in_specs=[pl.BlockSpec(memory_space=pltpu.VMEM)] * 3 + [pl.BlockSpec(memory_space=pltpu.SMEM)],
            out_specs=pl.BlockSpec(memory_space=pltpu.VMEM),
            scratch_shapes=[pltpu.VMEM((RATES, LANES), f32)]
            + [pltpu.VMEM((counts[lv], heights[lv], LANES), f32) for lv in range(bits)]
            + [pltpu.VMEM((len(level), up((rows >> (lv + 1)) * wide) + 2 * SUB, LANES), f32) for lv, (_, level) in enumerate(levels[:-1])]
            + [pltpu.VMEM((paths, chunks + 2 * SUB, LANES), f32)],
            compiler_params=pltpu.CompilerParams(vmem_limit_bytes=VMEM_LIMIT),
            cost_estimate=pl.CostEstimate(flops=INSIDE_FLOPS, bytes_accessed=4 * paths * chunks * LANES, transcendentals=0),
            name="inside",
        )(x, low, high, end)

    return call


def edges(rows, chunks):
    half = RATES // 2
    levels = plan(rows)
    bits = len(levels)

    def up(n):
        return -(-n // SUB) * SUB

    def at(start):
        return pl.ds(start, SUB)

    heights = [up((rows >> lv) * 2) + SUB for lv in range(bits)]
    counts = [2 * half * ((1 << lv) - 1) + 2 for lv in range(bits)]

    def kernel(lo_ref, hi_ref, stage_ref, stage, out_ref, sems, *bufs):
        trees, turns = bufs[:bits], bufs[bits:]
        lane = lax.broadcasted_iota(jnp.int32, (SUB, LANES), 1)
        none = jnp.zeros((1, LANES), jnp.float32)
        for t in range(rows):
            r = 2 * reverse(t, bits)
            trees[0][0, pl.ds(r, 1), :] = lo_ref[pl.ds(t, 1), :]
            trees[0][0, pl.ds(r + 1, 1), :] = none
            trees[0][1, pl.ds(r, 1), :] = none
            trees[0][1, pl.ds(r + 1, 1), :] = hi_ref[pl.ds(t, 1), :]

        def place(key, m, above):
            return key + half * (m - 1) + above

        def shifted(turn, w, r, s):
            if s > 0:
                return lax.select(lane < LANES - s, turn[w, at(SUB + r), :], turn[w, at(SUB + r + 1), :])
            return lax.select(lane >= -s, turn[w, at(SUB + r), :], turn[w, at(SUB + r - 1), :])

        for lv, (m, level) in enumerate(levels[:-1]):
            src, dst, turn = trees[lv], trees[lv + 1], turns[lv]
            n = (rows >> (lv + 1)) * 2
            sides = [(key, child, s, 0) for key, child, s in level if key <= 0]
            sides += [(key, child, s, 1) for key, child, s in level if key >= 0]
            for key, child, s, above in sides:
                a, w = place(child, m, above), place(key, 2 * m, above)
                for r in range(0, n, SUB):
                    v = src[a, at(n + r), :]
                    if s:
                        turn[w, at(SUB + r), :] = pltpu.roll(v, -s % LANES, 1)
                for r in range(0, n, SUB):
                    v = shifted(turn, w, r, s) if s else src[a, at(n + r), :]
                    dst[w, at(r), :] = src[a, at(r), :] + v

        m = levels[-1][0]
        src, turn = trees[-1], turns[-1]
        copies = []
        for q in range(-half, half):
            above = int(q >= 0)
            for d in range(rows):
                w = (q + half) * rows + d
                s = q * m + d - d // 2
                a = place(q * (m - 1) + d // 2, m, above)
                v = src[a, at(2), :]
                if s:
                    turn[w, at(SUB), :] = pltpu.roll(v, -s % LANES, 1)
                    v = shifted(turn, w, 0, s)
                v = src[a, at(0), :] + v
                row, k = (0, chunks - 1) if above else (1, 0)
                stage[w, pl.ds(k, 1), :] = stage_ref[w, pl.ds(k, 1), :] + v[row : row + 1]
            part = pl.ds((q + half) * rows, rows)
            copy = pltpu.make_async_copy(stage.at[part], out_ref.at[part], sems.at[q + half])
            copy.start()
            copies.append(copy)
        for copy in copies:
            copy.wait()

    def call(lo, hi, stage):
        f32 = jnp.float32
        paths = RATES * rows
        shape = jax.ShapeDtypeStruct((paths, chunks, LANES), f32)
        return pl.pallas_call(
            kernel,
            out_shape=(shape, shape),
            in_specs=[pl.BlockSpec(memory_space=pltpu.VMEM)] * 3,
            out_specs=(pl.BlockSpec(memory_space=pltpu.VMEM), pl.BlockSpec(memory_space=pl.ANY)),
            scratch_shapes=[pltpu.SemaphoreType.DMA((RATES,))]
            + [pltpu.VMEM((counts[lv], heights[lv], LANES), f32) for lv in range(bits)]
            + [pltpu.VMEM((counts[lv + 1], up((rows >> (lv + 1)) * 2) + 2 * SUB, LANES), f32) for lv in range(bits - 1)]
            + [pltpu.VMEM((paths, 3 * SUB, LANES), f32)],
            input_output_aliases={2: 0},
            compiler_params=pltpu.CompilerParams(vmem_limit_bytes=VMEM_LIMIT),
            name="edges",
        )(lo, hi, stage)[1]

    return call


def exchange(value, axes, partner):
    pairs = [(i, partner(i)) for i in range(lax.axis_size(axes))]
    return lax.ppermute(value, axes, [(i, j) for i, j in pairs if j is not None])


def search(spectra):
    rows, _, columns = spectra.shape
    chunks = columns // LANES
    half = chunks // 2
    x = spectra.reshape(rows, chunks, LANES)
    channels = lax.axis_size("coarse") * spectra.shape[1]
    band = ("coarse", "fine")
    place = lax.axis_index(band)
    side = lax.axis_index("coarse") % 2
    upper = side == 1

    own, given = lax.optimization_barrier(
        (jnp.where(upper, x[:, half:], x[:, :half]), jnp.where(upper, x[:, :half], x[:, half:]))
    )
    total = own + exchange(given, "coarse", lambda i: i ^ 1)

    count = lax.axis_size(band)
    odd = place % 2 == 1
    first = jnp.where(upper, given[:, 0], own[:, 0])
    last = jnp.where(upper, own[:, -1], given[:, -1])
    even_rim = exchange(jnp.where(odd, first, last), band, lambda i: i ^ 1)
    odd_rim = exchange(jnp.where(odd, last, first), band, lambda i: (i + (1 if i % 2 else -1)) % count)
    rim = jnp.stack([jnp.where(odd, even_rim, odd_rim), jnp.where(odd, odd_rim, even_rim)])
    rim_sum = rim
    for cross in (1, 6, 2):
        rim_sum = rim_sum + exchange(rim_sum, "coarse", lambda i: i ^ cross)
    inside_band = jnp.stack([place > 0, place < count - 1])[:, None, None]
    rim = jnp.where(inside_band, rim * (1.0 / (rim_sum / channels)) - 1.0, 0.0)

    for near, far in ((6, 2), (2, 6)):
        total = total + exchange(total, "coarse", lambda i: i ^ (far if i % 2 else near))
    other = exchange(total, "coarse", lambda i: i ^ 1)
    low, high = jnp.where(upper, other, total), jnp.where(upper, total, other)
    at_end = (place == count - 1).astype(jnp.int32).reshape(1)
    stage = inside(rows, chunks, channels)(x, low, high, at_end)
    out = edges(rows, chunks)(rim[0], rim[1], stage)
    return out.reshape(RATES, rows, 1, columns)


def solution(mesh):
    in_specs = (P(None, ("band", "coarse"), "fine"),)
    out_specs = P(None, None, ("band", "coarse"), "fine")
    return jax.shard_map(search, mesh=mesh, in_specs=in_specs, out_specs=out_specs, check_vma=False)
```

```python
import jax
import jax.numpy as jnp
from jax import lax
from jax.experimental import pallas as pl
from jax.experimental.pallas import tpu as pltpu
from jax.sharding import PartitionSpec as P


RATES = 8
LANES = 128
SUB = 8
VMEM_LIMIT = 36 * 1024 * 1024
INSIDE_FLOPS = 40_000_000


def reverse(i, bits):
    return int(format(i, f"0{bits}b")[::-1], 2)


def plan(rows):
    half, levels, m = RATES // 2, [], 1
    while m < rows:
        size = 2 * m
        level = []
        for key in range(-half * (size - 1), half * (size - 1) + 1):
            q = min(key // (size - 1), half - 1)
            d = key - q * (size - 1)
            level.append((key, q * (m - 1) + d // 2, q * m + d - d // 2))
        levels.append((m, level))
        m = size
    return levels


def inside(rows, chunks, channels):
    half = RATES // 2
    levels = plan(rows)
    bits = len(levels)
    wide = chunks + 2

    def up(n):
        return -(-n // SUB) * SUB

    heights = [up((rows >> lv) * wide) + SUB for lv in range(bits)]
    counts = [2 * half * ((1 << lv) - 1) + 1 for lv in range(bits)]

    def at(start):
        return pl.ds(start, SUB)

    def kernel(x_ref, low_ref, high_ref, end_ref, stage, fixed, *bufs):
        trees, turns = bufs[:bits], bufs[bits:]
        lane = lax.broadcasted_iota(jnp.int32, (SUB, LANES), 1)
        line = lane + LANES * lax.broadcasted_iota(jnp.int32, (SUB, LANES), 0)

        none = jnp.zeros((1, LANES), jnp.float32)
        base = trees[0]
        for t in range(rows):
            r = reverse(t, bits) * wide
            base[0, pl.ds(r, 1), :] = none
            for k in range(0, chunks, SUB):
                sums = low_ref if k < chunks // 2 else high_ref
                inverse = 1.0 / (sums[t, at(k % (chunks // 2)), :] / channels)
                base[0, at(r + 1 + k), :] = x_ref[t, at(k), :] * inverse - 1.0
            base[0, pl.ds(r + 1 + chunks, 1), :] = none

        def grow(lv, m, level):
            src, dst, turn = trees[lv], trees[lv + 1], turns[lv]
            n = (rows >> (lv + 1)) * wide
            for w, (key, child, s) in enumerate(level):
                a, o = child + half * (m - 1), key + half * (2 * m - 1)
                if s:
                    for r in range(0, n, SUB):
                        turn[w, at(SUB + r), :] = pltpu.roll(src[a, at(n + r), :], -s % LANES, 1)
                for r in range(0, n, SUB):
                    if s == 0:
                        v = src[a, at(n + r), :]
                    elif s > 0:
                        v = lax.select(lane < LANES - s, turn[w, at(SUB + r), :], turn[w, at(SUB + r + 1), :])
                    else:
                        v = lax.select(lane >= -s, turn[w, at(SUB + r), :], turn[w, at(SUB + r - 1), :])
                    dst[o, at(r), :] = src[a, at(r), :] + v

        for lv, (m, level) in enumerate(levels[:-1]):
            grow(lv, m, level)

        m = levels[-1][0]
        src, turn = trees[-1], turns[-1]

        def finish(q):
            for d in range(rows):
                w = (q + half) * rows + d
                s = q * m + d - d // 2
                a = q * (m - 1) + d // 2 + half * (m - 1)
                vs = [src[a, at(wide + 1 + k), :] for k in range(0, chunks, SUB)]
                if s > 0:
                    vs[0] = lax.select(line < s, src[a, at(wide + 1 + chunks), :], vs[0])
                if s < 0:
                    vs[-1] = lax.select(line >= SUB * LANES + s, src[a, at(wide + 1 - SUB), :], vs[-1])
                if s:
                    vs = [pltpu.roll(v, -s % LANES, 1) for v in vs]
                    for i, v in enumerate(vs):
                        turn[w, at(SUB + SUB * i), :] = v
                    if s > 0:
                        turn[w, at(SUB + chunks), :] = vs[0]
                        vs = [lax.select(lane < LANES - s, v, turn[w, at(SUB + SUB * i + 1), :]) for i, v in enumerate(vs)]
                    else:
                        turn[w, at(0), :] = vs[-1]
                        vs = [lax.select(lane >= -s, v, turn[w, at(SUB + SUB * i - 1), :]) for i, v in enumerate(vs)]
                for i, v in enumerate(vs):
                    stage[w, at(SUB * i), :] = src[a, at(1 + SUB * i), :] + v

        for q in range(-half, 0):
            finish(q)

        @pl.when(end_ref[0] > 0)
        def _():
            rate = lax.broadcasted_iota(jnp.int32, (RATES, LANES), 0)
            slope = half - 1 - rate
            blocks = []
            for t in range(rows):
                r = reverse(t, bits) * wide + 1 + chunks
                parts = []
                for k in (2, 1):
                    v = base[0, pl.ds(r - k, 1), :]
                    if t:
                        v = pltpu.roll(v, LANES - (half - 1) * t, 1)
                    v = jnp.broadcast_to(v, (RATES, LANES))
                    step = t
                    if (RATES - 1) * t >= LANES:
                        v = pltpu.roll(v, 0, 1, stride=SUB * 2, stride_axis=0)
                        step = t - SUB * 2
                    if step:
                        v = pltpu.roll(v, 0, 1, stride=step, stride_axis=0)
                    parts.append(v)
                where = lane + slope * t
                v = jnp.where(where < 0, parts[0], jnp.where(where < LANES, parts[1], 0.0))
                blocks.append([v])
            while len(blocks) > 1:
                joined = []
                for first, second in zip(blocks[0::2], blocks[1::2]):
                    block = []
                    for d in range(2 * len(first)):
                        s, v = d - d // 2, second[d // 2]
                        if s:
                            v = jnp.where(lane < LANES - s, pltpu.roll(v, LANES - s, 1), 0.0)
                        block.append(first[d // 2] + v)
                    joined.append(block)
                blocks = joined
            for d in range(rows):
                fixed[...] = blocks[0][d]
                for q in range(-half, 0):
                    stage[(q + half) * rows + d, pl.ds(chunks - 1, 1), :] = fixed[pl.ds(half - 1 - q, 1), :]

        for q in range(half):
            finish(q)

    def call(x, low, high, end):
        f32 = jnp.float32
        paths = RATES * rows
        return pl.pallas_call(
            kernel,
            out_shape=jax.ShapeDtypeStruct((paths, chunks, LANES), f32),
            in_specs=[pl.BlockSpec(memory_space=pltpu.VMEM)] * 3 + [pl.BlockSpec(memory_space=pltpu.SMEM)],
            out_specs=pl.BlockSpec(memory_space=pltpu.VMEM),
            scratch_shapes=[pltpu.VMEM((RATES, LANES), f32)]
            + [pltpu.VMEM((counts[lv], heights[lv], LANES), f32) for lv in range(bits)]
            + [pltpu.VMEM((len(level), up((rows >> (lv + 1)) * wide) + 2 * SUB, LANES), f32) for lv, (_, level) in enumerate(levels[:-1])]
            + [pltpu.VMEM((paths, chunks + 2 * SUB, LANES), f32)],
            compiler_params=pltpu.CompilerParams(vmem_limit_bytes=VMEM_LIMIT),
            cost_estimate=pl.CostEstimate(flops=INSIDE_FLOPS, bytes_accessed=4 * paths * chunks * LANES, transcendentals=0),
            name="inside",
        )(x, low, high, end)

    return call


def edges(rows, chunks):
    half = RATES // 2
    levels = plan(rows)
    bits = len(levels)

    def up(n):
        return -(-n // SUB) * SUB

    def at(start):
        return pl.ds(start, SUB)

    heights = [up((rows >> lv) * 2) + SUB for lv in range(bits)]
    counts = [2 * half * ((1 << lv) - 1) + 2 for lv in range(bits)]

    def kernel(lo_ref, hi_ref, stage_ref, stage, out_ref, sems, *bufs):
        trees, turns = bufs[:bits], bufs[bits:]
        lane = lax.broadcasted_iota(jnp.int32, (SUB, LANES), 1)
        none = jnp.zeros((1, LANES), jnp.float32)
        for t in range(rows):
            r = 2 * reverse(t, bits)
            trees[0][0, pl.ds(r, 1), :] = lo_ref[pl.ds(t, 1), :]
            trees[0][0, pl.ds(r + 1, 1), :] = none
            trees[0][1, pl.ds(r, 1), :] = none
            trees[0][1, pl.ds(r + 1, 1), :] = hi_ref[pl.ds(t, 1), :]

        def place(key, m, above):
            return key + half * (m - 1) + above

        def shifted(turn, w, r, s):
            if s > 0:
                return lax.select(lane < LANES - s, turn[w, at(SUB + r), :], turn[w, at(SUB + r + 1), :])
            return lax.select(lane >= -s, turn[w, at(SUB + r), :], turn[w, at(SUB + r - 1), :])

        for lv, (m, level) in enumerate(levels[:-1]):
            src, dst, turn = trees[lv], trees[lv + 1], turns[lv]
            n = (rows >> (lv + 1)) * 2
            sides = [(key, child, s, 0) for key, child, s in level if key <= 0]
            sides += [(key, child, s, 1) for key, child, s in level if key >= 0]
            for key, child, s, above in sides:
                a, w = place(child, m, above), place(key, 2 * m, above)
                for r in range(0, n, SUB):
                    v = src[a, at(n + r), :]
                    if s:
                        turn[w, at(SUB + r), :] = pltpu.roll(v, -s % LANES, 1)
                for r in range(0, n, SUB):
                    v = shifted(turn, w, r, s) if s else src[a, at(n + r), :]
                    dst[w, at(r), :] = src[a, at(r), :] + v

        m = levels[-1][0]
        src, turn = trees[-1], turns[-1]
        copies = []
        for q in range(-half, half):
            above = int(q >= 0)
            for d in range(rows):
                w = (q + half) * rows + d
                s = q * m + d - d // 2
                a = place(q * (m - 1) + d // 2, m, above)
                v = src[a, at(2), :]
                if s:
                    turn[w, at(SUB), :] = pltpu.roll(v, -s % LANES, 1)
                    v = shifted(turn, w, 0, s)
                v = src[a, at(0), :] + v
                row, k = (0, chunks - 1) if above else (1, 0)
                stage[w, pl.ds(k, 1), :] = stage_ref[w, pl.ds(k, 1), :] + v[row : row + 1]
            part = pl.ds((q + half) * rows, rows)
            copy = pltpu.make_async_copy(stage.at[part], out_ref.at[part], sems.at[q + half])
            copy.start()
            copies.append(copy)
        for copy in copies:
            copy.wait()

    def call(lo, hi, stage):
        f32 = jnp.float32
        paths = RATES * rows
        shape = jax.ShapeDtypeStruct((paths, chunks, LANES), f32)
        return pl.pallas_call(
            kernel,
            out_shape=(shape, shape),
            in_specs=[pl.BlockSpec(memory_space=pltpu.VMEM)] * 3,
            out_specs=(pl.BlockSpec(memory_space=pltpu.VMEM), pl.BlockSpec(memory_space=pl.ANY)),
            scratch_shapes=[pltpu.SemaphoreType.DMA((RATES,))]
            + [pltpu.VMEM((counts[lv], heights[lv], LANES), f32) for lv in range(bits)]
            + [pltpu.VMEM((counts[lv + 1], up((rows >> (lv + 1)) * 2) + 2 * SUB, LANES), f32) for lv in range(bits - 1)]
            + [pltpu.VMEM((paths, 3 * SUB, LANES), f32)],
            input_output_aliases={2: 0},
            compiler_params=pltpu.CompilerParams(vmem_limit_bytes=VMEM_LIMIT),
            name="edges",
        )(lo, hi, stage)[1]

    return call


def exchange(value, axes, partner):
    pairs = [(i, partner(i)) for i in range(lax.axis_size(axes))]
    return lax.ppermute(value, axes, [(i, j) for i, j in pairs if j is not None])


def search(spectra):
    rows, _, columns = spectra.shape
    chunks = columns // LANES
    half = chunks // 2
    x = spectra.reshape(rows, chunks, LANES)
    channels = lax.axis_size("coarse") * spectra.shape[1]
    band = ("coarse", "fine")
    place = lax.axis_index(band)
    side = lax.axis_index("coarse") % 2
    upper = side == 1

    own, given = lax.optimization_barrier(
        (jnp.where(upper, x[:, half:], x[:, :half]), jnp.where(upper, x[:, :half], x[:, half:]))
    )
    total = own + exchange(given, "coarse", lambda i: i ^ 1)

    count = lax.axis_size(band)
    odd = place % 2 == 1
    first = jnp.where(upper, given[:, 0], own[:, 0])
    last = jnp.where(upper, own[:, -1], given[:, -1])
    even_rim = exchange(jnp.where(odd, first, last), band, lambda i: i ^ 1)
    odd_rim = exchange(jnp.where(odd, last, first), band, lambda i: (i + (1 if i % 2 else -1)) % count)
    rim = jnp.stack([jnp.where(odd, even_rim, odd_rim), jnp.where(odd, odd_rim, even_rim)])
    pair = rim + exchange(rim, "coarse", lambda i: i ^ 1)
    rim_sum = pair
    for cross in (2, 6, 4):
        rim_sum = rim_sum + exchange(pair, "coarse", lambda i: i ^ cross)
    inside_band = jnp.stack([place > 0, place < count - 1])[:, None, None]
    rim = jnp.where(inside_band, rim * (1.0 / (rim_sum / channels)) - 1.0, 0.0)

    for near, far in ((6, 2), (2, 6)):
        total = total + exchange(total, "coarse", lambda i: i ^ (far if i % 2 else near))
    other = exchange(total, "coarse", lambda i: i ^ 1)
    low, high = jnp.where(upper, other, total), jnp.where(upper, total, other)
    at_end = (place == count - 1).astype(jnp.int32).reshape(1)
    stage = inside(rows, chunks, channels)(x, low, high, at_end)
    out = edges(rows, chunks)(rim[0], rim[1], stage)
    return out.reshape(RATES, rows, 1, columns)


def solution(mesh):
    in_specs = (P(None, ("band", "coarse"), "fine"),)
    out_specs = P(None, None, ("band", "coarse"), "fine")
    return jax.shard_map(search, mesh=mesh, in_specs=in_specs, out_specs=out_specs, check_vma=False)
```

```python
import jax
import jax.numpy as jnp
from jax import lax
from jax.experimental import pallas as pl
from jax.experimental.pallas import tpu as pltpu
from jax.sharding import PartitionSpec as P


RATES = 8
LANES = 128
SUB = 8
VMEM_LIMIT = 36 * 1024 * 1024
INSIDE_FLOPS = 40_000_000


def reverse(i, bits):
    return int(format(i, f"0{bits}b")[::-1], 2)


def plan(rows):
    half, levels, m = RATES // 2, [], 1
    while m < rows:
        size = 2 * m
        level = []
        for key in range(-half * (size - 1), half * (size - 1) + 1):
            q = min(key // (size - 1), half - 1)
            d = key - q * (size - 1)
            level.append((key, q * (m - 1) + d // 2, q * m + d - d // 2))
        levels.append((m, level))
        m = size
    return levels


def inside(rows, chunks, channels):
    half = RATES // 2
    levels = plan(rows)
    bits = len(levels)
    wide = chunks + 2

    def up(n):
        return -(-n // SUB) * SUB

    heights = [up((rows >> lv) * wide) + SUB for lv in range(bits)]
    counts = [2 * half * ((1 << lv) - 1) + 1 for lv in range(bits)]

    def at(start):
        return pl.ds(start, SUB)

    def kernel(x_ref, low_ref, high_ref, end_ref, stage, fixed, *bufs):
        trees, turns = bufs[:bits], bufs[bits:]
        lane = lax.broadcasted_iota(jnp.int32, (SUB, LANES), 1)
        line = lane + LANES * lax.broadcasted_iota(jnp.int32, (SUB, LANES), 0)

        none = jnp.zeros((1, LANES), jnp.float32)
        base = trees[0]
        for t in range(rows):
            r = reverse(t, bits) * wide
            base[0, pl.ds(r, 1), :] = none
            for k in range(0, chunks, SUB):
                sums = low_ref if k < chunks // 2 else high_ref
                inverse = 1.0 / (sums[t, at(k % (chunks // 2)), :] / channels)
                base[0, at(r + 1 + k), :] = x_ref[t, at(k), :] * inverse - 1.0
            base[0, pl.ds(r + 1 + chunks, 1), :] = none

        def grow(lv, m, level):
            src, dst, turn = trees[lv], trees[lv + 1], turns[lv]
            n = (rows >> (lv + 1)) * wide
            for w, (key, child, s) in enumerate(level):
                a, o = child + half * (m - 1), key + half * (2 * m - 1)
                if s:
                    for r in range(0, n, SUB):
                        turn[w, at(SUB + r), :] = pltpu.roll(src[a, at(n + r), :], -s % LANES, 1)
                for r in range(0, n, SUB):
                    if s == 0:
                        v = src[a, at(n + r), :]
                    elif s > 0:
                        v = lax.select(lane < LANES - s, turn[w, at(SUB + r), :], turn[w, at(SUB + r + 1), :])
                    else:
                        v = lax.select(lane >= -s, turn[w, at(SUB + r), :], turn[w, at(SUB + r - 1), :])
                    dst[o, at(r), :] = src[a, at(r), :] + v

        for lv, (m, level) in enumerate(levels[:-1]):
            grow(lv, m, level)

        m = levels[-1][0]
        src, turn = trees[-1], turns[-1]

        def finish(q):
            for d in range(rows):
                w = (q + half) * rows + d
                s = q * m + d - d // 2
                a = q * (m - 1) + d // 2 + half * (m - 1)
                vs = [src[a, at(wide + 1 + k), :] for k in range(0, chunks, SUB)]
                if s > 0:
                    vs[0] = lax.select(line < s, src[a, at(wide + 1 + chunks), :], vs[0])
                if s < 0:
                    vs[-1] = lax.select(line >= SUB * LANES + s, src[a, at(wide + 1 - SUB), :], vs[-1])
                if s:
                    vs = [pltpu.roll(v, -s % LANES, 1) for v in vs]
                    for i, v in enumerate(vs):
                        turn[w, at(SUB + SUB * i), :] = v
                    if s > 0:
                        turn[w, at(SUB + chunks), :] = vs[0]
                        vs = [lax.select(lane < LANES - s, v, turn[w, at(SUB + SUB * i + 1), :]) for i, v in enumerate(vs)]
                    else:
                        turn[w, at(0), :] = vs[-1]
                        vs = [lax.select(lane >= -s, v, turn[w, at(SUB + SUB * i - 1), :]) for i, v in enumerate(vs)]
                for i, v in enumerate(vs):
                    stage[w, at(SUB * i), :] = src[a, at(1 + SUB * i), :] + v

        for q in range(-half, 0):
            finish(q)

        @pl.when(end_ref[0] > 0)
        def _():
            rate = lax.broadcasted_iota(jnp.int32, (RATES, LANES), 0)
            slope = half - 1 - rate
            blocks = []
            for t in range(rows):
                r = reverse(t, bits) * wide + 1 + chunks
                parts = []
                for k in (2, 1):
                    v = base[0, pl.ds(r - k, 1), :]
                    if t:
                        v = pltpu.roll(v, LANES - (half - 1) * t, 1)
                    v = jnp.broadcast_to(v, (RATES, LANES))
                    step = t
                    if (RATES - 1) * t >= LANES:
                        v = pltpu.roll(v, 0, 1, stride=SUB * 2, stride_axis=0)
                        step = t - SUB * 2
                    if step:
                        v = pltpu.roll(v, 0, 1, stride=step, stride_axis=0)
                    parts.append(v)
                where = lane + slope * t
                v = jnp.where(where < 0, parts[0], jnp.where(where < LANES, parts[1], 0.0))
                blocks.append([v])
            while len(blocks) > 1:
                joined = []
                for first, second in zip(blocks[0::2], blocks[1::2]):
                    block = []
                    for d in range(2 * len(first)):
                        s, v = d - d // 2, second[d // 2]
                        if s:
                            v = jnp.where(lane < LANES - s, pltpu.roll(v, LANES - s, 1), 0.0)
                        block.append(first[d // 2] + v)
                    joined.append(block)
                blocks = joined
            for d in range(rows):
                fixed[...] = blocks[0][d]
                for q in range(-half, 0):
                    stage[(q + half) * rows + d, pl.ds(chunks - 1, 1), :] = fixed[pl.ds(half - 1 - q, 1), :]

        for q in range(half):
            finish(q)

    def call(x, low, high, end):
        f32 = jnp.float32
        paths = RATES * rows
        return pl.pallas_call(
            kernel,
            out_shape=jax.ShapeDtypeStruct((paths, chunks, LANES), f32),
            in_specs=[pl.BlockSpec(memory_space=pltpu.VMEM)] * 3 + [pl.BlockSpec(memory_space=pltpu.SMEM)],
            out_specs=pl.BlockSpec(memory_space=pltpu.VMEM),
            scratch_shapes=[pltpu.VMEM((RATES, LANES), f32)]
            + [pltpu.VMEM((counts[lv], heights[lv], LANES), f32) for lv in range(bits)]
            + [pltpu.VMEM((len(level), up((rows >> (lv + 1)) * wide) + 2 * SUB, LANES), f32) for lv, (_, level) in enumerate(levels[:-1])]
            + [pltpu.VMEM((paths, chunks + 2 * SUB, LANES), f32)],
            compiler_params=pltpu.CompilerParams(vmem_limit_bytes=VMEM_LIMIT),
            cost_estimate=pl.CostEstimate(flops=INSIDE_FLOPS, bytes_accessed=4 * paths * chunks * LANES, transcendentals=0),
            name="inside",
        )(x, low, high, end)

    return call


def edges(rows, chunks):
    half = RATES // 2
    levels = plan(rows)
    bits = len(levels)

    def up(n):
        return -(-n // SUB) * SUB

    def at(start):
        return pl.ds(start, SUB)

    heights = [up((rows >> lv) * 2) + SUB for lv in range(bits)]
    counts = [2 * half * ((1 << lv) - 1) + 2 for lv in range(bits)]

    def kernel(lo_ref, hi_ref, stage_ref, stage, out_ref, sems, *bufs):
        trees, turns = bufs[:bits], bufs[bits:]
        lane = lax.broadcasted_iota(jnp.int32, (SUB, LANES), 1)
        none = jnp.zeros((1, LANES), jnp.float32)
        for t in range(rows):
            r = 2 * reverse(t, bits)
            trees[0][0, pl.ds(r, 1), :] = lo_ref[pl.ds(t, 1), :]
            trees[0][0, pl.ds(r + 1, 1), :] = none
            trees[0][1, pl.ds(r, 1), :] = none
            trees[0][1, pl.ds(r + 1, 1), :] = hi_ref[pl.ds(t, 1), :]

        def place(key, m, above):
            return key + half * (m - 1) + above

        def shifted(turn, w, r, s):
            if s > 0:
                return lax.select(lane < LANES - s, turn[w, at(SUB + r), :], turn[w, at(SUB + r + 1), :])
            return lax.select(lane >= -s, turn[w, at(SUB + r), :], turn[w, at(SUB + r - 1), :])

        for lv, (m, level) in enumerate(levels[:-1]):
            src, dst, turn = trees[lv], trees[lv + 1], turns[lv]
            n = (rows >> (lv + 1)) * 2
            sides = [(key, child, s, 0) for key, child, s in level if key <= 0]
            sides += [(key, child, s, 1) for key, child, s in level if key >= 0]
            for key, child, s, above in sides:
                a, w = place(child, m, above), place(key, 2 * m, above)
                for r in range(0, n, SUB):
                    v = src[a, at(n + r), :]
                    if s:
                        turn[w, at(SUB + r), :] = pltpu.roll(v, -s % LANES, 1)
                for r in range(0, n, SUB):
                    v = shifted(turn, w, r, s) if s else src[a, at(n + r), :]
                    dst[w, at(r), :] = src[a, at(r), :] + v

        m = levels[-1][0]
        src, turn = trees[-1], turns[-1]
        copies = []
        for q in range(-half, half):
            above = int(q >= 0)
            for d in range(rows):
                w = (q + half) * rows + d
                s = q * m + d - d // 2
                a = place(q * (m - 1) + d // 2, m, above)
                v = src[a, at(2), :]
                if s:
                    turn[w, at(SUB), :] = pltpu.roll(v, -s % LANES, 1)
                    v = shifted(turn, w, 0, s)
                v = src[a, at(0), :] + v
                row, k = (0, chunks - 1) if above else (1, 0)
                stage[w, pl.ds(k, 1), :] = stage_ref[w, pl.ds(k, 1), :] + v[row : row + 1]
            part = pl.ds((q + half) * rows, rows)
            copy = pltpu.make_async_copy(stage.at[part], out_ref.at[part], sems.at[q + half])
            copy.start()
            copies.append(copy)
        for copy in copies:
            copy.wait()

    def call(lo, hi, stage):
        f32 = jnp.float32
        paths = RATES * rows
        shape = jax.ShapeDtypeStruct((paths, chunks, LANES), f32)
        return pl.pallas_call(
            kernel,
            out_shape=(shape, shape),
            in_specs=[pl.BlockSpec(memory_space=pltpu.VMEM)] * 3,
            out_specs=(pl.BlockSpec(memory_space=pltpu.VMEM), pl.BlockSpec(memory_space=pl.ANY)),
            scratch_shapes=[pltpu.SemaphoreType.DMA((RATES,))]
            + [pltpu.VMEM((counts[lv], heights[lv], LANES), f32) for lv in range(bits)]
            + [pltpu.VMEM((counts[lv + 1], up((rows >> (lv + 1)) * 2) + 2 * SUB, LANES), f32) for lv in range(bits - 1)]
            + [pltpu.VMEM((paths, 3 * SUB, LANES), f32)],
            input_output_aliases={2: 0},
            compiler_params=pltpu.CompilerParams(vmem_limit_bytes=VMEM_LIMIT),
            name="edges",
        )(lo, hi, stage)[1]

    return call


def exchange(value, axes, partner):
    pairs = [(i, partner(i)) for i in range(lax.axis_size(axes))]
    return lax.ppermute(value, axes, [(i, j) for i, j in pairs if j is not None])


def search(spectra):
    rows, _, columns = spectra.shape
    chunks = columns // LANES
    half = chunks // 2
    x = spectra.reshape(rows, chunks, LANES)
    channels = lax.axis_size("coarse") * spectra.shape[1]
    band = ("coarse", "fine")
    place = lax.axis_index(band)
    side = lax.axis_index("coarse") % 2
    upper = side == 1

    own, given = lax.optimization_barrier(
        (jnp.where(upper, x[:, half:], x[:, :half]), jnp.where(upper, x[:, :half], x[:, half:]))
    )
    total = own + exchange(given, "coarse", lambda i: i ^ 1)

    count = lax.axis_size(band)
    odd = place % 2 == 1
    first = jnp.where(upper, given[:, 0], own[:, 0])
    last = jnp.where(upper, own[:, -1], given[:, -1])
    even_rim = exchange(jnp.where(odd, first, last), band, lambda i: i ^ 1)
    odd_rim = exchange(jnp.where(odd, last, first), band, lambda i: (i + (1 if i % 2 else -1)) % count)
    rim = jnp.stack([jnp.where(odd, even_rim, odd_rim), jnp.where(odd, odd_rim, even_rim)])
    pair = rim + exchange(rim, "coarse", lambda i: i ^ 1)
    rim_sum = pair
    for cross in (2, 6, 4):
        rim_sum = rim_sum + exchange(pair, "coarse", lambda i: i ^ cross)
    rim = rim * (1.0 / (rim_sum / channels)) - 1.0
    before = jnp.where(place > 0, rim[0], 0.0)
    after = jnp.where(place < count - 1, rim[1], 0.0)

    for near, far in ((6, 2), (2, 6)):
        total = total + exchange(total, "coarse", lambda i: i ^ (far if i % 2 else near))
    other = exchange(total, "coarse", lambda i: i ^ 1)
    low, high = jnp.where(upper, other, total), jnp.where(upper, total, other)
    at_end = (place == count - 1).astype(jnp.int32).reshape(1)
    stage = inside(rows, chunks, channels)(x, low, high, at_end)
    out = edges(rows, chunks)(before, after, stage)
    return out.reshape(RATES, rows, 1, columns)


def solution(mesh):
    in_specs = (P(None, ("band", "coarse"), "fine"),)
    out_specs = P(None, None, ("band", "coarse"), "fine")
    return jax.shard_map(search, mesh=mesh, in_specs=in_specs, out_specs=out_specs, check_vma=False)
```
